32 devices in a mesh: blk: 8 (over y, x, core), grp: 4 (over z).
Axes of the slice: x: 2, y: 2, z: 4, core: 2. Of those that a mesh axis runs over, the one named last changes fastest.
Arguments:
- amplitudes: bfloat16 [896, 4, 896], P('blk', None, 'grp'), may hold values from -6 to 6
- grid_factor: bfloat16 [1024, 896], P(('blk', 'grp')), may hold values from -0.1875 to 0.1875
- metric: float32 [1024, 4, 256], P('blk', 'grp'), may hold values from -6 to 6
- virt_energy: float32 [896], replicated, may hold values from 0.2 to 4
- pair_energy: float32 [4], replicated, may hold values from -2 to -0.5
Outputs:
- residual: float32 [896, 4, 896], P('blk', None, 'grp')
The draws below stay inside these ranges and needn't reach their ends.
All inputs are finite; a program needn't handle non-finite values.
Results may differ from the reference program's by a relative error of at most 0.005.
Values may be sent and summed in bfloat16 or wider, within the bound.
A program may use at most 64 MiB of HBM per device.

```python
import math
import jax
import jax.numpy as jnp
from jax import lax

NV = 896
PTS = 32
OP = 4
NG = 1024
N_BLK = 8
N_GRP = 4


def block_levels(stream_key, extent, pieces, least, top_value):
    gain = 1.0
    for position, blocks in pieces:
        heights = jax.random.uniform(jax.random.fold_in(jax.random.fold_in(stream_key, 6), position), (blocks,), jnp.float32, least / len(pieces), top_value / len(pieces))
        gain = gain * jnp.repeat(jnp.exp(heights), extent[position] // blocks).reshape((-1,) + (1,) * (len(extent) - 1 - position))
    return gain


def normal_values(stream_key, extent, width, most, cuts=(), kind=jnp.bfloat16):
    result = jax.random.normal(stream_key, extent, jnp.float32) * width
    if len(cuts) > 0:
        result = block_levels(stream_key, extent, cuts, -0.22, 0.18) * result
    return jnp.clip(result, min=-most, max=most).astype(kind)


def setup_inputs(seed: int = 0) -> dict:
    key_list = jax.random.split(jax.random.key(seed), 6)
    return {
        "amplitudes": normal_values(key_list[0], (NV, OP, NV), 1.0, 6.0, ((0, 8), (2, 4))),
        "grid_factor": normal_values(key_list[1], (NG, NV), NV ** -0.5, 0.1875, ((0, 32),)),
        "metric": normal_values(key_list[2], (NG, N_GRP, N_BLK * PTS), ((NG // NV) ** 2) ** -0.5, 6.0, ((0, 8), (1, 4)), jnp.float32),
        "virt_energy": jnp.clip(jnp.exp(jax.random.uniform(key_list[3], (NV,), jnp.float32, math.log(0.2), math.log(4.0))), 0.2, 4.0),
        "pair_energy": jnp.clip(jax.random.uniform(key_list[4], (OP,), jnp.float32, -2.0, -0.5), -2.0, -0.5),
    }


def reference(amplitudes, grid_factor, metric, virt_energy, pair_energy):
    metric_full = jnp.transpose(metric.reshape(NG, N_GRP, N_BLK, PTS), (0, 2, 1, 3)).reshape(NG, NG)
    factor_split = grid_factor.reshape(N_BLK, N_GRP, PTS, NV)

    def one_pair(pair_amp):
        left = jnp.dot(grid_factor, pair_amp, preferred_element_type=jnp.float32).astype(jnp.bfloat16)
        products = jnp.dot(left, grid_factor.T, preferred_element_type=jnp.float32)
        weighted = (metric_full * products).astype(jnp.bfloat16).reshape(NG, N_BLK, N_GRP, PTS)

        def add_group(summed, group):
            block = lax.dynamic_index_in_dim(weighted, group, 2, keepdims=False).astype(jnp.float32)
            rows = lax.dynamic_index_in_dim(factor_split, group, 1, keepdims=False).astype(jnp.float32)
            partial_sum = jnp.einsum("pbr,brv->pv", block, rows, precision=lax.Precision.HIGHEST)
            rounded = lax.optimization_barrier(partial_sum.astype(jnp.bfloat16))
            return summed + rounded.astype(jnp.float32), None

        summed, unused = lax.scan(add_group, jnp.zeros((NG, NV), jnp.float32), jnp.arange(N_GRP, dtype=jnp.int32))
        mixed = summed.astype(jnp.bfloat16)
        return jnp.dot(grid_factor.T, mixed, preferred_element_type=jnp.float32)

    ladder = lax.map(one_pair, jnp.transpose(amplitudes, (1, 0, 2)))
    ladder = jnp.transpose(ladder, (1, 0, 2))
    denominator = virt_energy[:, None, None] + virt_energy[None, None, :] - pair_energy[None, :, None]
    return denominator * amplitudes.astype(jnp.float32) + ladder
```

```python
import functools

import jax
import jax.numpy as jnp
from jax import lax
from jax.experimental import pallas as pl
from jax.experimental.pallas import tpu as pltpu
from jax.sharding import PartitionSpec as P


def local(amplitudes, grid_factor, metric, virt_energy, pair_energy):
    row_factor = lax.all_gather(grid_factor, "grp", axis=0, tiled=True)
    column_factor = lax.all_gather(grid_factor, "blk", axis=0, tiled=True)
    amplitude_rows = lax.all_gather(amplitudes, "blk", axis=0, tiled=True)
    row_count = row_factor.shape[0]
    left_part = jnp.einsum(
        "pc,ckd->kpd", row_factor, amplitude_rows, preferred_element_type=jnp.float32
    ).astype(jnp.bfloat16)
    columns = column_factor
    products = jnp.einsum(
        "kpd,qd->kpq",
        lax.all_gather(left_part, "grp", axis=2, tiled=True),
        columns,
        preferred_element_type=jnp.float32,
    )
    weighted = (metric.reshape(row_count, -1)[None] * products).astype(jnp.bfloat16)
    columns = column_factor
    mixed = lax.psum_scatter(
        jnp.einsum("kpq,qb->bkp", weighted, columns, preferred_element_type=jnp.float32).astype(
            jnp.bfloat16
        ),
        "grp",
        scatter_dimension=0,
        tiled=True,
    )
    columns = row_factor
    ladder = lax.psum_scatter(
        jnp.einsum("pa,bkp->akb", columns, mixed, preferred_element_type=jnp.float32).astype(
            jnp.bfloat16
        ),
        "blk",
        scatter_dimension=0,
        tiled=True,
    ).astype(jnp.float32)
    first_energy = lax.dynamic_slice_in_dim(
        virt_energy, lax.axis_index("blk") * amplitudes.shape[0], amplitudes.shape[0]
    )
    second_energy = lax.dynamic_slice_in_dim(
        virt_energy, lax.axis_index("grp") * amplitudes.shape[2], amplitudes.shape[2]
    )
    denominator = (
        first_energy[:, None, None] + second_energy[None, None, :] - pair_energy[None, :, None]
    )
    return denominator * amplitudes.astype(jnp.float32) + ladder


MESH = pl.DeviceIdType.MESH
F32 = jnp.float32
BF16 = jnp.bfloat16


def flip(index, mask):
    bit = 1
    while bit <= mask:
        if mask & bit:
            index = index + bit - 2 * bit * lax.rem(lax.div(index, bit), 2)
        bit *= 2
    return index


def column_chunks(total, width):
    return [(start, min(width, total - start)) for start in range(0, total, width)]


def kernel(
    n_blk, n_grp, t_ref, x_ref, z_ref, o_ref,
    factor, pieces, amps, weights, left, mixed, ladder, out_send, out_recv,
    z_send_sem, z_recv_sem, p_send_sem, p_recv_sem, o_send_sem, o_recv_sem,
):
    me = lax.axis_index("blk")
    grp = lax.axis_index("grp")
    pairs, rows, cols = t_ref.shape
    points, virtuals = x_ref.shape
    even = list(range(2, n_blk, 2))
    direct = even + [1]
    started = []

    def peer(step):
        return lax.rem(grp + step, n_grp)

    barrier = pltpu.get_barrier_semaphore()
    for step in range(1, n_grp):
        pl.semaphore_signal(barrier, inc=1, device_id={"grp": peer(step)}, device_id_type=MESH)
    for mask in direct:
        pl.semaphore_signal(barrier, inc=1, device_id={"blk": flip(me, mask)}, device_id_type=MESH)
    pl.semaphore_wait(barrier, n_grp - 1 + len(direct))

    def rows_of(source, size):
        return pl.ds(pl.multiple_of(source * size, size), size)

    def z_copy(kind, step, src, dst):
        return pltpu.make_async_remote_copy(
            src_ref=src, dst_ref=dst,
            send_sem=z_send_sem.at[kind, step], recv_sem=z_recv_sem.at[kind, step],
            device_id={"grp": peer(step)}, device_id_type=MESH,
        )

    def z_dst(kind, source):
        if kind == 0:
            return factor.at[source, rows_of(me, points), :]
        return (pieces if kind == 1 else weights).at[source]

    def z_start(kind, step):
        src = (x_ref, t_ref.at[peer(step)], z_ref)[kind]
        copy = z_copy(kind, step, src, z_dst(kind, grp))
        copy.start()
        started.append(copy)

    def z_wait(kind, step):
        dst = z_dst(kind, peer(n_grp - step))
        z_copy(kind, step, dst, dst).wait_recv()

    chunks = column_chunks(virtuals, -(-cols // 128) * 128)

    def region(item, source):
        if item < n_grp:
            return factor.at[peer((n_grp - item) % n_grp), rows_of(source, points), :]
        if item == n_grp:
            return amps.at[rows_of(source, rows), :]
        start, width = chunks[item - n_grp - 1]
        return mixed.at[:, rows_of(source, points), pl.ds(start, width)]

    def p_copy(item, mask, hop, src=None):
        place = region(item, flip(me, mask))
        return pltpu.make_async_remote_copy(
            src_ref=place if src is None else src, dst_ref=place,
            send_sem=p_send_sem.at[item, mask ^ hop], recv_sem=p_recv_sem.at[item, mask ^ hop],
            device_id={"blk": flip(me, hop)}, device_id_type=MESH,
        )

    def p_wait(item, mask):
        place = region(item, flip(me, mask))
        pltpu.make_async_remote_copy(
            src_ref=place, dst_ref=place,
            send_sem=p_send_sem.at[item, mask], recv_sem=p_recv_sem.at[item, mask],
            device_id={"blk": flip(me, mask)}, device_id_type=MESH,
        ).wait_recv()

    def p_spread(item, src=None):
        for mask in direct:
            copy = p_copy(item, 0, mask, src)
            copy.start()
            started.append(copy)

    def p_forward(item):
        for mask in even:
            p_wait(item, mask)
            copy = p_copy(item, mask, 1)
            copy.start()
            started.append(copy)

    def p_rest(item):
        for mask in range(1, n_blk, 2):
            p_wait(item, mask)

    for step in range(1, n_grp):
        z_start(0, step)
    p_spread(0, x_ref)
    for kind in (1, 2):
        for step in range(1, n_grp):
            z_start(kind, step)
    factor[grp, rows_of(me, points), :] = x_ref[...]
    pieces[grp] = t_ref[grp]
    weights[grp] = z_ref[...]
    for step in range(1, n_grp):
        z_wait(0, step)
        p_spread(step)
    for step in range(1, n_grp):
        z_wait(1, step)
    for g in range(n_grp):
        amps[rows_of(me, rows), g * cols:(g + 1) * cols] = pieces[g]
    p_spread(n_grp)
    for item in range(n_grp + 1):
        p_forward(item)
    for item in range(n_grp + 1):
        p_rest(item)
    for step in range(1, n_grp):
        z_wait(2, step)

    own = factor[:, rows_of(me, points), :].reshape(n_grp * points, virtuals)
    left[...] = jnp.dot(own, amps[...], preferred_element_type=F32).astype(BF16)
    weighted = []
    for g in range(n_grp):
        products = lax.dot_general(
            left[...], factor[g], (((1,), (1,)), ((), ())), preferred_element_type=F32
        )
        weighted.append((weights[g].astype(F32) * products).astype(BF16))
    weighted = jnp.concatenate(weighted, axis=1)
    total = n_grp * n_blk * points
    for number, (start, width) in enumerate(chunks):
        part = jnp.dot(
            weighted, factor[:, :, start:start + width].reshape(total, width),
            preferred_element_type=F32,
        ).astype(BF16)
        mixed[:, rows_of(me, points), start:start + width] = part.reshape(n_grp, points, width)
        p_spread(n_grp + 1 + number)

    picked = lax.broadcasted_iota(jnp.int32, (rows, virtuals), 1) == (
        lax.broadcasted_iota(jnp.int32, (rows, virtuals), 0) + me * rows
    )
    picked = picked.astype(F32).astype(BF16)
    columns = lax.dot_general(
        picked, factor[...].reshape(total, virtuals), (((1,), (1,)), ((), ())),
        preferred_element_type=F32,
    ).astype(BF16)

    def o_copy(target, source):
        return pltpu.make_async_remote_copy(
            src_ref=out_send.at[target], dst_ref=out_recv.at[source],
            send_sem=o_send_sem.at[target], recv_sem=o_recv_sem.at[source],
            device_id={"grp": target}, device_id_type=MESH,
        )

    done = 0
    for number, (start, width) in enumerate(chunks):
        p_forward(n_grp + 1 + number)
        p_rest(n_grp + 1 + number)
        ladder[:, start:start + width] = jnp.dot(
            columns, mixed[:, :, start:start + width].reshape(total, width),
            preferred_element_type=F32,
        )
        while done < n_grp and (done + 1) * cols <= start + width:
            block = ladder[:, done * cols:(done + 1) * cols].astype(BF16)
            out_send[done] = block

            @pl.when(grp != done)
            def _(target=done):
                o_copy(target, grp).start()

            done += 1
    for step in range(1, n_grp):
        source = peer(step)
        o_copy(source, source).wait_recv()
        o_ref[source] = out_recv[source]
    o_ref[grp] = out_send[grp]
    for target in range(n_grp):
        @pl.when(grp != target)
        def _(target=target):
            o_copy(target, grp).wait_send()
    for copy in started:
        copy.wait_send()


def ladder_term(n_blk, n_grp, amps, factor_rows, weights):
    pairs, rows, cols = amps.shape
    points, virtuals = factor_rows.shape
    items = n_grp + 1 + len(column_chunks(virtuals, -(-cols // 128) * 128))
    dma = pltpu.SemaphoreType.DMA
    vmem = pl.BlockSpec(memory_space=pltpu.VMEM)
    return pl.pallas_call(
        functools.partial(kernel, n_blk, n_grp),
        out_shape=jax.ShapeDtypeStruct(amps.shape, BF16),
        in_specs=[vmem] * 3,
        out_specs=vmem,
        scratch_shapes=[
            pltpu.VMEM((n_grp, n_blk * points, virtuals), BF16),
            pltpu.VMEM((n_grp, rows, cols), BF16),
            pltpu.VMEM((n_blk * rows, virtuals), BF16),
            pltpu.VMEM((n_grp,) + weights.shape, BF16),
            pltpu.VMEM((n_grp * points, virtuals), BF16),
            pltpu.VMEM((n_grp, n_blk * points, virtuals), BF16),
            pltpu.VMEM((rows, virtuals), F32),
            pltpu.VMEM((n_grp, rows, cols), BF16),
            pltpu.VMEM((n_grp, rows, cols), BF16),
            dma((3, n_grp)), dma((3, n_grp)),
            dma((items, n_blk)), dma((items, n_blk)),
            dma((n_grp,)), dma((n_grp,)),
        ],
        compiler_params=pltpu.CompilerParams(collective_id=0, has_side_effects=True),
    )(amps, factor_rows, weights)


def denominators(amplitudes, virt_energy, pair_energy):
    first_energy = lax.dynamic_slice_in_dim(
        virt_energy, lax.axis_index("blk") * amplitudes.shape[0], amplitudes.shape[0]
    )
    second_energy = lax.dynamic_slice_in_dim(
        virt_energy, lax.axis_index("grp") * amplitudes.shape[2], amplitudes.shape[2]
    )
    return first_energy[:, None, None] + second_energy[None, None, :] - pair_energy[None, :, None]


def by_pair(n_blk, n_grp, amplitudes, grid_factor, metric, virt_energy, pair_energy):
    ladder = ladder_term(
        n_blk, n_grp, jnp.transpose(amplitudes, (1, 0, 2)), grid_factor, metric[:, 0].astype(BF16)
    )
    denominator = denominators(amplitudes, virt_energy, pair_energy)
    return denominator * amplitudes.astype(F32) + jnp.transpose(ladder, (1, 0, 2)).astype(F32)


def solution(mesh):
    in_specs = (P("blk", None, "grp"), P(("blk", "grp"), None), P("blk", "grp", None), P(), P())
    out_specs = P("blk", None, "grp")
    n_blk, n_grp = mesh.shape["blk"], mesh.shape["grp"]

    def body(amplitudes, *rest):
        rows, pairs, cols = amplitudes.shape
        points, virtuals = rest[0].shape
        fits = pairs == n_grp and n_blk & (n_blk - 1) == 0 and n_blk >= 4
        fits = fits and rows % 16 == 0 and points % 16 == 0 and virtuals % 128 == 0
        if fits:
            return by_pair(n_blk, n_grp, amplitudes, *rest)
        return local(amplitudes, *rest)

    return jax.shard_map(body, mesh=mesh, in_specs=in_specs, out_specs=out_specs, check_vma=False)
```

```python
import functools

import jax
import jax.numpy as jnp
from jax import lax
from jax.experimental import pallas as pl
from jax.experimental.pallas import tpu as pltpu
from jax.sharding import PartitionSpec as P


def local(amplitudes, grid_factor, metric, virt_energy, pair_energy):
    row_factor = lax.all_gather(grid_factor, "grp", axis=0, tiled=True)
    column_factor = lax.all_gather(grid_factor, "blk", axis=0, tiled=True)
    amplitude_rows = lax.all_gather(amplitudes, "blk", axis=0, tiled=True)
    row_count = row_factor.shape[0]
    left_part = jnp.einsum(
        "pc,ckd->kpd", row_factor, amplitude_rows, preferred_element_type=jnp.float32
    ).astype(jnp.bfloat16)
    columns = column_factor
    products = jnp.einsum(
        "kpd,qd->kpq",
        lax.all_gather(left_part, "grp", axis=2, tiled=True),
        columns,
        preferred_element_type=jnp.float32,
    )
    weighted = (metric.reshape(row_count, -1)[None] * products).astype(jnp.bfloat16)
    columns = column_factor
    mixed = lax.psum_scatter(
        jnp.einsum("kpq,qb->bkp", weighted, columns, preferred_element_type=jnp.float32).astype(
            jnp.bfloat16
        ),
        "grp",
        scatter_dimension=0,
        tiled=True,
    )
    columns = row_factor
    ladder = lax.psum_scatter(
        jnp.einsum("pa,bkp->akb", columns, mixed, preferred_element_type=jnp.float32).astype(
            jnp.bfloat16
        ),
        "blk",
        scatter_dimension=0,
        tiled=True,
    ).astype(jnp.float32)
    first_energy = lax.dynamic_slice_in_dim(
        virt_energy, lax.axis_index("blk") * amplitudes.shape[0], amplitudes.shape[0]
    )
    second_energy = lax.dynamic_slice_in_dim(
        virt_energy, lax.axis_index("grp") * amplitudes.shape[2], amplitudes.shape[2]
    )
    denominator = (
        first_energy[:, None, None] + second_energy[None, None, :] - pair_energy[None, :, None]
    )
    return denominator * amplitudes.astype(jnp.float32) + ladder


MESH = pl.DeviceIdType.MESH
F32 = jnp.float32
BF16 = jnp.bfloat16


def flip(index, mask):
    bit = 1
    while bit <= mask:
        if mask & bit:
            index = index + bit - 2 * bit * lax.rem(lax.div(index, bit), 2)
        bit *= 2
    return index


def column_chunks(total, width):
    return [(start, min(width, total - start)) for start in range(0, total, width)]


def kernel(
    n_blk, n_grp, t_ref, x_ref, z_ref, o_ref,
    factor, pieces, amps, weights, left, mixed, ladder, out_send, out_recv,
    z_send_sem, z_recv_sem, p_send_sem, p_recv_sem, o_send_sem, o_recv_sem,
):
    me = lax.axis_index("blk")
    grp = lax.axis_index("grp")
    pairs, rows, cols = t_ref.shape
    points, virtuals = x_ref.shape
    core, near, far = 1, 2, 4
    direct = [near, far, core]
    started = []

    def peer(step):
        return lax.rem(grp + step, n_grp)

    barrier = pltpu.get_barrier_semaphore()
    for step in range(1, n_grp):
        pl.semaphore_signal(barrier, inc=1, device_id={"grp": peer(step)}, device_id_type=MESH)
    for mask in direct:
        pl.semaphore_signal(barrier, inc=1, device_id={"blk": flip(me, mask)}, device_id_type=MESH)
    pl.semaphore_wait(barrier, n_grp - 1 + len(direct))

    def rows_of(source, size):
        return pl.ds(pl.multiple_of(source * size, size), size)

    def z_copy(kind, step, src, dst):
        return pltpu.make_async_remote_copy(
            src_ref=src, dst_ref=dst,
            send_sem=z_send_sem.at[kind, step], recv_sem=z_recv_sem.at[kind, step],
            device_id={"grp": peer(step)}, device_id_type=MESH,
        )

    def z_dst(kind, source):
        if kind == 0:
            return factor.at[source, rows_of(me, points), :]
        return (pieces if kind == 1 else weights).at[source]

    def z_start(kind, step):
        src = (x_ref, t_ref.at[peer(step)], z_ref)[kind]
        copy = z_copy(kind, step, src, z_dst(kind, grp))
        copy.start()
        started.append(copy)

    def z_wait(kind, step):
        dst = z_dst(kind, peer(n_grp - step))
        z_copy(kind, step, dst, dst).wait_recv()

    chunks = column_chunks(virtuals, -(-cols // 128) * 128)

    def region(item, half, source):
        if item < n_grp:
            part = points // 2
            begin = pl.multiple_of(source * points + half * part, part)
            return factor.at[peer((n_grp - item) % n_grp), pl.ds(begin, part), :]
        if item == n_grp:
            part = -(-rows // 32) * 16
            size = part if half == 0 else rows - part
            begin = pl.multiple_of(source * rows + half * part, 16)
            return amps.at[pl.ds(begin, size), :]
        start, width = chunks[item - n_grp - 1]
        part = n_grp // 2
        return mixed.at[pl.ds(half * part, part), rows_of(source, points), pl.ds(start, width)]

    def p_copy(item, half, mask, hop, src=None):
        place = region(item, half, flip(me, mask))
        return pltpu.make_async_remote_copy(
            src_ref=place if src is None else src, dst_ref=place,
            send_sem=p_send_sem.at[item, half, mask ^ hop],
            recv_sem=p_recv_sem.at[item, half, mask ^ hop],
            device_id={"blk": flip(me, hop)}, device_id_type=MESH,
        )

    def p_send(item, half, mask, hop, src=None):
        copy = p_copy(item, half, mask, hop, src)
        copy.start()
        started.append(copy)

    def p_wait(item, half, mask):
        p_copy(item, half, mask, 0).wait_recv()

    def p_spread(item, src=None):
        sources = (None, None)
        if src is not None:
            part = points // 2
            sources = tuple(src.at[half * part:(half + 1) * part, :] for half in range(2))
        for turn in range(2):
            p_send(item, turn, 0, near, sources[turn])
            p_send(item, 1 - turn, 0, far, sources[1 - turn])
        for half in range(2):
            p_send(item, half, 0, core, sources[half])

    def p_relay(item):
        for turn in range(2):
            for mask, half, onward in ((near, turn, far), (far, 1 - turn, near)):
                p_wait(item, half, mask)
                if turn == 0:
                    p_send(item, half, mask, onward)
                p_send(item, half, mask, core)

    def p_across(item):
        for half in range(2):
            p_wait(item, half, near + far)
            p_send(item, half, near + far, core)

    def p_rest(item):
        for mask in range(1, n_blk, 2):
            for half in range(2):
                p_wait(item, half, mask)

    for step in range(1, n_grp):
        z_start(0, step)
    p_spread(0, x_ref)
    for kind in (1, 2):
        for step in range(1, n_grp):
            z_start(kind, step)
    factor[grp, rows_of(me, points), :] = x_ref[...]
    pieces[grp] = t_ref[grp]
    weights[grp] = z_ref[...]
    for step in range(1, n_grp):
        z_wait(0, step)
        p_spread(step)
        p_relay(step - 1)
    p_relay(n_grp - 1)
    for step in range(1, n_grp):
        z_wait(1, step)
    for g in range(n_grp):
        amps[rows_of(me, rows), g * cols:(g + 1) * cols] = pieces[g]
    p_spread(n_grp)
    for item in range(n_grp):
        p_across(item)
    p_relay(n_grp)
    p_across(n_grp)
    for item in range(n_grp + 1):
        p_rest(item)
    for step in range(1, n_grp):
        z_wait(2, step)

    own = factor[:, rows_of(me, points), :].reshape(n_grp * points, virtuals)
    left[...] = jnp.dot(own, amps[...], preferred_element_type=F32).astype(BF16)
    weighted = []
    for g in range(n_grp):
        products = lax.dot_general(
            left[...], factor[g], (((1,), (1,)), ((), ())), preferred_element_type=F32
        )
        weighted.append((weights[g].astype(F32) * products).astype(BF16))
    weighted = jnp.concatenate(weighted, axis=1)
    total = n_grp * n_blk * points
    for number, (start, width) in enumerate(chunks):
        part = jnp.dot(
            weighted, factor[:, :, start:start + width].reshape(total, width),
            preferred_element_type=F32,
        ).astype(BF16)
        mixed[:, rows_of(me, points), start:start + width] = part.reshape(n_grp, points, width)
        p_spread(n_grp + 1 + number)

    picked = lax.broadcasted_iota(jnp.int32, (rows, virtuals), 1) == (
        lax.broadcasted_iota(jnp.int32, (rows, virtuals), 0) + me * rows
    )
    picked = picked.astype(F32).astype(BF16)
    columns = lax.dot_general(
        picked, factor[...].reshape(total, virtuals), (((1,), (1,)), ((), ())),
        preferred_element_type=F32,
    ).astype(BF16)

    def o_copy(target, source):
        return pltpu.make_async_remote_copy(
            src_ref=out_send.at[target], dst_ref=out_recv.at[source],
            send_sem=o_send_sem.at[target], recv_sem=o_recv_sem.at[source],
            device_id={"grp": target}, device_id_type=MESH,
        )

    ready = [0]

    def finish(number):
        start, width = chunks[number]
        p_across(n_grp + 1 + number)
        p_rest(n_grp + 1 + number)
        ladder[:, start:start + width] = jnp.dot(
            columns, mixed[:, :, start:start + width].reshape(total, width),
            preferred_element_type=F32,
        )
        while ready[0] < n_grp and (ready[0] + 1) * cols <= start + width:
            target = ready[0]
            out_send[target] = ladder[:, target * cols:(target + 1) * cols].astype(BF16)

            @pl.when(grp != target)
            def _(target=target):
                o_copy(target, grp).start()

            ready[0] += 1

    for number in range(len(chunks)):
        p_relay(n_grp + 1 + number)
        if number > 0:
            finish(number - 1)
    finish(len(chunks) - 1)
    for step in range(1, n_grp):
        source = peer(step)
        o_copy(source, source).wait_recv()
        o_ref[source] = out_recv[source]
    o_ref[grp] = out_send[grp]
    for target in range(n_grp):
        @pl.when(grp != target)
        def _(target=target):
            o_copy(target, grp).wait_send()
    for copy in started:
        copy.wait_send()


def ladder_term(n_blk, n_grp, amps, factor_rows, weights):
    pairs, rows, cols = amps.shape
    points, virtuals = factor_rows.shape
    items = n_grp + 1 + len(column_chunks(virtuals, -(-cols // 128) * 128))
    dma = pltpu.SemaphoreType.DMA
    vmem = pl.BlockSpec(memory_space=pltpu.VMEM)
    return pl.pallas_call(
        functools.partial(kernel, n_blk, n_grp),
        out_shape=jax.ShapeDtypeStruct(amps.shape, BF16),
        in_specs=[vmem] * 3,
        out_specs=vmem,
        scratch_shapes=[
            pltpu.VMEM((n_grp, n_blk * points, virtuals), BF16),
            pltpu.VMEM((n_grp, rows, cols), BF16),
            pltpu.VMEM((n_blk * rows, virtuals), BF16),
            pltpu.VMEM((n_grp,) + weights.shape, BF16),
            pltpu.VMEM((n_grp * points, virtuals), BF16),
            pltpu.VMEM((n_grp, n_blk * points, virtuals), BF16),
            pltpu.VMEM((rows, virtuals), F32),
            pltpu.VMEM((n_grp, rows, cols), BF16),
            pltpu.VMEM((n_grp, rows, cols), BF16),
            dma((3, n_grp)), dma((3, n_grp)),
            dma((items, 2, n_blk)), dma((items, 2, n_blk)),
            dma((n_grp,)), dma((n_grp,)),
        ],
        compiler_params=pltpu.CompilerParams(collective_id=0, has_side_effects=True),
    )(amps, factor_rows, weights)


def denominators(amplitudes, virt_energy, pair_energy):
    first_energy = lax.dynamic_slice_in_dim(
        virt_energy, lax.axis_index("blk") * amplitudes.shape[0], amplitudes.shape[0]
    )
    second_energy = lax.dynamic_slice_in_dim(
        virt_energy, lax.axis_index("grp") * amplitudes.shape[2], amplitudes.shape[2]
    )
    return first_energy[:, None, None] + second_energy[None, None, :] - pair_energy[None, :, None]


def by_pair(n_blk, n_grp, amplitudes, grid_factor, metric, virt_energy, pair_energy):
    ladder = ladder_term(
        n_blk, n_grp, jnp.transpose(amplitudes, (1, 0, 2)), grid_factor, metric[:, 0].astype(BF16)
    )
    denominator = denominators(amplitudes, virt_energy, pair_energy)
    return denominator * amplitudes.astype(F32) + jnp.transpose(ladder, (1, 0, 2)).astype(F32)


def solution(mesh):
    in_specs = (P("blk", None, "grp"), P(("blk", "grp"), None), P("blk", "grp", None), P(), P())
    out_specs = P("blk", None, "grp")
    n_blk, n_grp = mesh.shape["blk"], mesh.shape["grp"]

    def body(amplitudes, *rest):
        rows, pairs, cols = amplitudes.shape
        points, virtuals = rest[0].shape
        fits = pairs == n_grp and n_grp % 2 == 0 and n_blk == 8
        fits = fits and rows % 16 == 0 and points % 32 == 0 and virtuals % 128 == 0
        if fits:
            return by_pair(n_blk, n_grp, amplitudes, *rest)
        return local(amplitudes, *rest)

    return jax.shard_map(body, mesh=mesh, in_specs=in_specs, out_specs=out_specs, check_vma=False)
```

```python
import functools

import jax
import jax.numpy as jnp
from jax import lax
from jax.experimental import pallas as pl
from jax.experimental.pallas import tpu as pltpu
from jax.sharding import PartitionSpec as P


def local(amplitudes, grid_factor, metric, virt_energy, pair_energy):
    row_factor = lax.all_gather(grid_factor, "grp", axis=0, tiled=True)
    column_factor = lax.all_gather(grid_factor, "blk", axis=0, tiled=True)
    amplitude_rows = lax.all_gather(amplitudes, "blk", axis=0, tiled=True)
    row_count = row_factor.shape[0]
    left_part = jnp.einsum(
        "pc,ckd->kpd", row_factor, amplitude_rows, preferred_element_type=jnp.float32
    ).astype(jnp.bfloat16)
    columns = column_factor
    products = jnp.einsum(
        "kpd,qd->kpq",
        lax.all_gather(left_part, "grp", axis=2, tiled=True),
        columns,
        preferred_element_type=jnp.float32,
    )
    weighted = (metric.reshape(row_count, -1)[None] * products).astype(jnp.bfloat16)
    columns = column_factor
    mixed = lax.psum_scatter(
        jnp.einsum("kpq,qb->bkp", weighted, columns, preferred_element_type=jnp.float32).astype(
            jnp.bfloat16
        ),
        "grp",
        scatter_dimension=0,
        tiled=True,
    )
    columns = row_factor
    ladder = lax.psum_scatter(
        jnp.einsum("pa,bkp->akb", columns, mixed, preferred_element_type=jnp.float32).astype(
            jnp.bfloat16
        ),
        "blk",
        scatter_dimension=0,
        tiled=True,
    ).astype(jnp.float32)
    first_energy = lax.dynamic_slice_in_dim(
        virt_energy, lax.axis_index("blk") * amplitudes.shape[0], amplitudes.shape[0]
    )
    second_energy = lax.dynamic_slice_in_dim(
        virt_energy, lax.axis_index("grp") * amplitudes.shape[2], amplitudes.shape[2]
    )
    denominator = (
        first_energy[:, None, None] + second_energy[None, None, :] - pair_energy[None, :, None]
    )
    return denominator * amplitudes.astype(jnp.float32) + ladder


MESH = pl.DeviceIdType.MESH
F32 = jnp.float32
BF16 = jnp.bfloat16


def flip(index, mask):
    bit = 1
    while bit <= mask:
        if mask & bit:
            index = index + bit - 2 * bit * lax.rem(lax.div(index, bit), 2)
        bit *= 2
    return index


def column_chunks(total, width):
    return [(start, min(width, total - start)) for start in range(0, total, width)]


def kernel(
    n_blk, n_grp, t_ref, x_ref, z_ref, e_ref, f_ref, o_ref,
    own_amps, own_weights, factor, pieces, amps, weights, left, mixed, ladder, out_send, out_recv,
    x_send_sem, x_recv_sem, z_send_sem, z_recv_sem, p_send_sem, p_recv_sem, o_send_sem, o_recv_sem,
):
    me = lax.axis_index("blk")
    grp = lax.axis_index("grp")
    rows, pairs, cols = t_ref.shape
    points, virtuals = x_ref.shape
    core, near, far = 1, 2, 4
    direct = [near, far, core]
    started = []

    def peer(step):
        return lax.rem(grp + step, n_grp)

    barrier = pltpu.get_barrier_semaphore()
    for step in range(1, n_grp):
        pl.semaphore_signal(barrier, inc=1, device_id={"grp": peer(step)}, device_id_type=MESH)
    for mask in direct:
        pl.semaphore_signal(barrier, inc=1, device_id={"blk": flip(me, mask)}, device_id_type=MESH)
    for pair in range(pairs):
        own_amps[pair] = t_ref[:, pair, :]
    own_weights[...] = z_ref[:, 0, :].astype(BF16)
    pl.semaphore_wait(barrier, n_grp - 1 + len(direct))

    def rows_of(source, size):
        return pl.ds(pl.multiple_of(source * size, size), size)

    mate, across = flip(grp, 1), n_grp - 1 - grp
    half_index = lax.div(grp, 2)
    inner = jnp.logical_and(grp > 0, grp < n_grp - 1)
    owners = (grp, mate, 2 - half_index, 3 - 3 * half_index)

    def x_copy(number, slot, owner, target, src=None):
        place = factor.at[owner, rows_of(me, points), :]
        return pltpu.make_async_remote_copy(
            src_ref=place if src is None else src, dst_ref=place,
            send_sem=x_send_sem.at[number], recv_sem=x_recv_sem.at[slot],
            device_id={"grp": target}, device_id_type=MESH,
        )

    def x_wait(slot):
        x_copy(0, slot, owners[slot], mate).wait_recv()

    x_sends = (
        lambda: x_copy(0, 1, grp, mate, x_ref),
        lambda: x_copy(1, 2, grp, across, x_ref),
        lambda: x_copy(2, 3, owners[1], across),
        lambda: x_copy(3, 2, owners[2], mate),
        lambda: x_copy(4, 3, owners[3], mate),
    )

    def x_pass(number):
        @pl.when(inner)
        def _():
            x_sends[number]().start()

    def z_copy(kind, step, src, dst):
        return pltpu.make_async_remote_copy(
            src_ref=src, dst_ref=dst,
            send_sem=z_send_sem.at[kind, step], recv_sem=z_recv_sem.at[kind, step],
            device_id={"grp": peer(step)}, device_id_type=MESH,
        )

    def z_dst(kind, source):
        return (pieces, weights)[kind].at[source]

    def z_start(kind, step):
        src = (own_amps.at[peer(step)], own_weights)[kind]
        copy = z_copy(kind, step, src, z_dst(kind, grp))
        copy.start()
        started.append(copy)

    def z_wait(kind, step):
        dst = z_dst(kind, peer(n_grp - step))
        z_copy(kind, step, dst, dst).wait_recv()

    chunks = column_chunks(virtuals, -(-cols // 128) * 128)

    def region(item, half, source):
        if item < n_grp:
            part = points // 2
            begin = pl.multiple_of(source * points + half * part, part)
            return factor.at[owners[item], pl.ds(begin, part), :]
        if item == n_grp:
            part = -(-rows // 32) * 16
            size = part if half == 0 else rows - part
            begin = pl.multiple_of(source * rows + half * part, 16)
            return amps.at[pl.ds(begin, size), :]
        number = item - n_grp - 1
        part = n_grp * points // 2
        begin = pl.multiple_of(source * 2 * part + half * part, part)
        return mixed.at[number, pl.ds(begin, part), pl.ds(0, chunks[number][1])]

    def p_copy(item, half, mask, hop, src=None):
        place = region(item, half, flip(me, mask))
        return pltpu.make_async_remote_copy(
            src_ref=place if src is None else src, dst_ref=place,
            send_sem=p_send_sem.at[item, half, mask ^ hop],
            recv_sem=p_recv_sem.at[item, half, mask ^ hop],
            device_id={"blk": flip(me, hop)}, device_id_type=MESH,
        )

    def p_send(item, half, mask, hop, src=None):
        copy = p_copy(item, half, mask, hop, src)
        copy.start()
        started.append(copy)

    def p_wait(item, half, mask):
        p_copy(item, half, mask, 0).wait_recv()

    def relayed(item):
        return item != n_grp + len(chunks)

    def p_spread(item, src=None):
        sources = (None, None)
        if src is not None:
            part = points // 2
            sources = tuple(src.at[half * part:(half + 1) * part, :] for half in range(2))
        for turn in range(2):
            p_send(item, turn, 0, near, sources[turn])
            p_send(item, 1 - turn, 0, far, sources[1 - turn])
        if not relayed(item):
            for half in range(2):
                p_send(item, half, 0, near + far, sources[half])
        for half in range(2):
            p_send(item, half, 0, core, sources[half])

    def p_relay(item):
        for turn in range(2):
            for mask, half, onward in ((near, turn, far), (far, 1 - turn, near)):
                p_wait(item, half, mask)
                if turn == 0 and relayed(item):
                    p_send(item, half, mask, onward)
                p_send(item, half, mask, core)

    def p_across(item):
        for half in range(2):
            p_wait(item, half, near + far)
            p_send(item, half, near + far, core)

    def p_rest(item):
        for mask in range(1, n_blk, 2):
            for half in range(2):
                p_wait(item, half, mask)

    x_sends[0]().start()
    x_pass(1)
    p_spread(0, x_ref)
    for step in range(1, n_grp):
        z_start(0, step)
    factor[grp, rows_of(me, points), :] = x_ref[...]
    pieces[grp] = own_amps[grp]
    weights[grp] = own_weights[...]
    x_wait(1)
    x_pass(2)
    p_spread(1)
    p_relay(0)
    x_wait(2)
    x_pass(3)
    p_spread(2)
    p_relay(1)

    @pl.when(inner)
    def _():
        x_wait(3)

    x_pass(4)
    for step in range(1, n_grp):
        z_start(1, step)
    for step in range(1, n_grp):
        z_wait(0, step)
    for g in range(n_grp):
        amps[rows_of(me, rows), g * cols:(g + 1) * cols] = pieces[g]
    p_spread(n_grp)
    p_relay(2)

    @pl.when(jnp.logical_not(inner))
    def _():
        x_wait(3)

    p_spread(3)
    for item in range(3):
        p_across(item)
    p_relay(n_grp)
    p_relay(3)
    p_across(n_grp)
    p_across(3)
    for item in range(n_grp + 1):
        p_rest(item)
    for step in range(1, n_grp):
        z_wait(1, step)

    own = factor[:, rows_of(me, points), :].reshape(n_grp * points, virtuals)
    left[...] = jnp.dot(own, amps[...], preferred_element_type=F32).astype(BF16)
    weighted = []
    for g in range(n_grp):
        products = lax.dot_general(
            left[...], factor[g], (((1,), (1,)), ((), ())), preferred_element_type=F32
        )
        weighted.append((weights[g].astype(F32) * products).astype(BF16))
    weighted = jnp.concatenate(weighted, axis=1)
    total = n_grp * n_blk * points
    for number, (start, width) in enumerate(chunks):
        part = jnp.dot(
            weighted, factor[:, :, start:start + width].reshape(total, width),
            preferred_element_type=F32,
        ).astype(BF16)
        mixed[number, rows_of(me, n_grp * points), :width] = part
        p_spread(n_grp + 1 + number)

    picked = lax.broadcasted_iota(jnp.int32, (rows, virtuals), 1) == (
        lax.broadcasted_iota(jnp.int32, (rows, virtuals), 0) + me * rows
    )
    energies = e_ref[...].reshape(1, virtuals)
    first_energy = jnp.sum(jnp.where(picked, energies, 0.0), axis=1, keepdims=True)
    second_energy = jnp.zeros((1, cols), F32)
    for g in range(n_grp):
        second_energy += jnp.where(grp == g, energies[:, g * cols:(g + 1) * cols], 0.0)
    energy_sum = first_energy + second_energy
    picked = picked.astype(F32).astype(BF16)
    by_owner = jnp.concatenate(
        [
            factor[:, block * points:(block + 1) * points, :].reshape(n_grp * points, virtuals)
            for block in range(n_blk)
        ],
        axis=0,
    )
    columns = lax.dot_general(
        picked, by_owner, (((1,), (1,)), ((), ())),
        preferred_element_type=F32,
    ).astype(BF16)

    def o_copy(target, source):
        return pltpu.make_async_remote_copy(
            src_ref=out_send.at[target], dst_ref=out_recv.at[source],
            send_sem=o_send_sem.at[target], recv_sem=o_recv_sem.at[source],
            device_id={"grp": target}, device_id_type=MESH,
        )

    ready = [0]

    def finish(number):
        start, width = chunks[number]
        p_across(n_grp + 1 + number)
        p_rest(n_grp + 1 + number)
        ladder[:, start:start + width] = jnp.dot(
            columns, mixed[number, :, :width],
            preferred_element_type=F32,
        )
        while ready[0] < n_grp and (ready[0] + 1) * cols <= start + width:
            target = ready[0]
            out_send[target] = ladder[:, target * cols:(target + 1) * cols].astype(BF16)

            @pl.when(grp != target)
            def _(target=target):
                o_copy(target, grp).start()

            ready[0] += 1

    ahead = 3
    for number in range(len(chunks) + ahead - 1):
        if number < len(chunks):
            p_relay(n_grp + 1 + number)
        if number >= ahead - 1:
            finish(number - ahead + 1)
    out_recv[grp] = out_send[grp]
    for pair in range(pairs):
        @pl.when(grp != pair)
        def _(pair=pair):
            o_copy(pair, pair).wait_recv()

        diagonal = (energy_sum - f_ref[pair]) * own_amps[pair].astype(F32)
        o_ref[pair] = diagonal + out_recv[pair].astype(F32)
    for target in range(n_grp):
        @pl.when(grp != target)
        def _(target=target):
            o_copy(target, grp).wait_send()
    for copy in started:
        copy.wait_send()
    x_sends[0]().wait_send()

    @pl.when(inner)
    def _():
        for send in x_sends[1:]:
            send().wait_send()


def by_pair(n_blk, n_grp, amplitudes, grid_factor, metric, virt_energy, pair_energy):
    rows, pairs, cols = amplitudes.shape
    points, virtuals = grid_factor.shape
    height, unused, width = metric.shape
    chunks = column_chunks(virtuals, -(-cols // 128) * 128)
    items = n_grp + 1 + len(chunks)
    dma = pltpu.SemaphoreType.DMA
    vmem = pl.BlockSpec(memory_space=pltpu.VMEM)
    residual = pl.pallas_call(
        functools.partial(kernel, n_blk, n_grp),
        out_shape=jax.ShapeDtypeStruct((pairs, rows, cols), F32),
        in_specs=[vmem] * 4 + [pl.BlockSpec(memory_space=pltpu.SMEM)],
        out_specs=vmem,
        scratch_shapes=[
            pltpu.VMEM((pairs, rows, cols), BF16),
            pltpu.VMEM((height, width), BF16),
            pltpu.VMEM((n_grp, n_blk * points, virtuals), BF16),
            pltpu.VMEM((n_grp, rows, cols), BF16),
            pltpu.VMEM((n_blk * rows, virtuals), BF16),
            pltpu.VMEM((n_grp, height, width), BF16),
            pltpu.VMEM((n_grp * points, virtuals), BF16),
            pltpu.VMEM((len(chunks), n_grp * n_blk * points, chunks[0][1]), BF16),
            pltpu.VMEM((rows, virtuals), F32),
            pltpu.VMEM((n_grp, rows, cols), BF16),
            pltpu.VMEM((n_grp, rows, cols), BF16),
            dma((5,)), dma((4,)), dma((2, n_grp)), dma((2, n_grp)),
            dma((items, 2, n_blk)), dma((items, 2, n_blk)),
            dma((n_grp,)), dma((n_grp,)),
        ],
        compiler_params=pltpu.CompilerParams(collective_id=0, has_side_effects=True),
    )(amplitudes, grid_factor, metric, virt_energy, pair_energy)
    return jnp.transpose(residual, (1, 0, 2))


def solution(mesh):
    in_specs = (P("blk", None, "grp"), P(("blk", "grp"), None), P("blk", "grp", None), P(), P())
    out_specs = P("blk", None, "grp")
    n_blk, n_grp = mesh.shape["blk"], mesh.shape["grp"]

    def body(amplitudes, *rest):
        rows, pairs, cols = amplitudes.shape
        points, virtuals = rest[0].shape
        fits = pairs == n_grp and n_grp == 4 and n_blk == 8
        fits = fits and rows % 16 == 0 and points % 32 == 0 and virtuals % 128 == 0
        if fits:
            return by_pair(n_blk, n_grp, amplitudes, *rest)
        return local(amplitudes, *rest)

    return jax.shard_map(body, mesh=mesh, in_specs=in_specs, out_specs=out_specs, check_vma=False)
```

```python
import functools

import jax
import jax.numpy as jnp
from jax import lax
from jax.experimental import pallas as pl
from jax.experimental.pallas import tpu as pltpu
from jax.sharding import PartitionSpec as P


def local(amplitudes, grid_factor, metric, virt_energy, pair_energy):
    row_factor = lax.all_gather(grid_factor, "grp", axis=0, tiled=True)
    column_factor = lax.all_gather(grid_factor, "blk", axis=0, tiled=True)
    amplitude_rows = lax.all_gather(amplitudes, "blk", axis=0, tiled=True)
    row_count = row_factor.shape[0]
    left_part = jnp.einsum(
        "pc,ckd->kpd", row_factor, amplitude_rows, preferred_element_type=jnp.float32
    ).astype(jnp.bfloat16)
    columns = column_factor
    products = jnp.einsum(
        "kpd,qd->kpq",
        lax.all_gather(left_part, "grp", axis=2, tiled=True),
        columns,
        preferred_element_type=jnp.float32,
    )
    weighted = (metric.reshape(row_count, -1)[None] * products).astype(jnp.bfloat16)
    columns = column_factor
    mixed = lax.psum_scatter(
        jnp.einsum("kpq,qb->bkp", weighted, columns, preferred_element_type=jnp.float32).astype(
            jnp.bfloat16
        ),
        "grp",
        scatter_dimension=0,
        tiled=True,
    )
    columns = row_factor
    ladder = lax.psum_scatter(
        jnp.einsum("pa,bkp->akb", columns, mixed, preferred_element_type=jnp.float32).astype(
            jnp.bfloat16
        ),
        "blk",
        scatter_dimension=0,
        tiled=True,
    ).astype(jnp.float32)
    first_energy = lax.dynamic_slice_in_dim(
        virt_energy, lax.axis_index("blk") * amplitudes.shape[0], amplitudes.shape[0]
    )
    second_energy = lax.dynamic_slice_in_dim(
        virt_energy, lax.axis_index("grp") * amplitudes.shape[2], amplitudes.shape[2]
    )
    denominator = (
        first_energy[:, None, None] + second_energy[None, None, :] - pair_energy[None, :, None]
    )
    return denominator * amplitudes.astype(jnp.float32) + ladder


MESH = pl.DeviceIdType.MESH
F32 = jnp.float32
BF16 = jnp.bfloat16


def flip(index, mask):
    bit = 1
    while bit <= mask:
        if mask & bit:
            index = index + bit - 2 * bit * lax.rem(lax.div(index, bit), 2)
        bit *= 2
    return index


def column_chunks(total, width):
    return [(start, min(width, total - start)) for start in range(0, total, width)]


def kernel(
    n_blk, n_grp, t_hbm, x_hbm, z_hbm, e_ref, f_ref, o_ref,
    t_ref, x_ref, z_ref, in_sem, own_amps, own_weights, factor, pieces, amps, weights, left, mixed, ladder, out_send, out_recv,
    z_send_sem, z_recv_sem, p_send_sem, p_recv_sem, o_send_sem, o_recv_sem,
):
    me = lax.axis_index("blk")
    grp = lax.axis_index("grp")
    rows, pairs, cols = t_ref.shape
    points, virtuals = x_ref.shape
    core, near, far = 1, 2, 4
    direct = [near, far, core]
    started = []

    def peer(step):
        return flip(grp, step)

    barrier = pltpu.get_barrier_semaphore()
    loads = [
        pltpu.make_async_copy(src, dst, in_sem.at[number])
        for number, (src, dst) in enumerate(
            ((t_hbm, t_ref), (z_hbm, z_ref), (x_hbm, x_ref))
        )
    ]
    for load in loads:
        load.start()
    for step in range(1, n_grp):
        pl.semaphore_signal(barrier, inc=1, device_id={"grp": peer(step)}, device_id_type=MESH)
    for mask in direct:
        pl.semaphore_signal(barrier, inc=1, device_id={"blk": flip(me, mask)}, device_id_type=MESH)
    loads[0].wait()
    for pair in range(pairs):
        own_amps[pair] = t_ref[:, pair, :]
    for load in loads[1:]:
        load.wait()
    own_weights[...] = z_ref[:, 0, :].astype(BF16)
    pl.semaphore_wait(barrier, n_grp - 1 + len(direct))

    def rows_of(source, size):
        return pl.ds(pl.multiple_of(source * size, size), size)

    cut = -(-rows // 32) * 16
    groups = ((0, cut), (cut, rows - cut))

    def z_copy(kind, step, src, dst):
        return pltpu.make_async_remote_copy(
            src_ref=src, dst_ref=dst,
            send_sem=z_send_sem.at[kind, step], recv_sem=z_recv_sem.at[kind, step],
            device_id={"grp": peer(step)}, device_id_type=MESH,
        )

    def z_dst(kind, source):
        if kind == 0:
            return factor.at[source, rows_of(me, points), :]
        if kind == 3:
            return weights.at[source]
        begin, size = groups[kind - 1]
        return pieces.at[source, begin:begin + size, :]

    def z_start(kind, step):
        if kind in (1, 2):
            begin, size = groups[kind - 1]
            src = own_amps.at[peer(step), begin:begin + size, :]
        else:
            src = x_ref if kind == 0 else own_weights
        copy = z_copy(kind, step, src, z_dst(kind, grp))
        copy.start()
        started.append(copy)

    def z_wait(kind, step):
        dst = z_dst(kind, peer(step))
        z_copy(kind, step, dst, dst).wait_recv()

    chunks = column_chunks(virtuals, -(-cols // 128) * 128)

    first = n_grp + len(groups)

    def region(item, half, source):
        if item < n_grp:
            part = points // 2
            begin = pl.multiple_of(source * points + half * part, part)
            return factor.at[peer(item), pl.ds(begin, part), :]
        if item < first:
            begin, size = groups[item - n_grp]
            part = -(-size // 32) * 16
            begin += half * part + source * rows
            return amps.at[pl.ds(pl.multiple_of(begin, 16), part if half == 0 else size - part), :]
        number = item - first
        part = n_grp * points // 2
        begin = pl.multiple_of(source * 2 * part + half * part, part)
        return mixed.at[number, pl.ds(begin, part), pl.ds(0, chunks[number][1])]

    def p_copy(item, half, mask, hop, src=None):
        place = region(item, half, flip(me, mask))
        return pltpu.make_async_remote_copy(
            src_ref=place if src is None else src, dst_ref=place,
            send_sem=p_send_sem.at[item, half, mask ^ hop],
            recv_sem=p_recv_sem.at[item, half, mask ^ hop],
            device_id={"blk": flip(me, hop)}, device_id_type=MESH,
        )

    def p_send(item, half, mask, hop, src=None):
        copy = p_copy(item, half, mask, hop, src)
        copy.start()
        started.append(copy)

    def p_wait(item, half, mask):
        p_copy(item, half, mask, 0).wait_recv()

    def relayed(item):
        return item != first + len(chunks) - 1

    def p_spread(item, src=None):
        sources = (None, None)
        if src is not None:
            part = points // 2
            sources = tuple(src.at[half * part:(half + 1) * part, :] for half in range(2))
        for turn in range(2):
            p_send(item, turn, 0, near, sources[turn])
            p_send(item, 1 - turn, 0, far, sources[1 - turn])
        if not relayed(item):
            for half in range(2):
                p_send(item, half, 0, near + far, sources[half])
        for half in range(2):
            p_send(item, half, 0, core, sources[half])

    def p_relay(item):
        for turn in range(2):
            for mask, half, onward in ((near, turn, far), (far, 1 - turn, near)):
                p_wait(item, half, mask)
                if turn == 0 and relayed(item):
                    p_send(item, half, mask, onward)
                p_send(item, half, mask, core)

    def p_across(item):
        for half in range(2):
            p_wait(item, half, near + far)
            p_send(item, half, near + far, core)

    def p_rest(item):
        for mask in range(1, n_blk, 2):
            for half in range(2):
                p_wait(item, half, mask)

    p_spread(0, x_ref)
    z_start(0, 1)
    for kind in (1, 2):
        for step in (1, 2, 3):
            z_start(kind, step)
    z_start(0, 3)
    z_start(0, 2)
    for step in (1, 2, 3):
        z_start(3, step)
    factor[grp, rows_of(me, points), :] = x_ref[...]
    pieces[grp] = own_amps[grp]
    weights[grp] = own_weights[...]
    z_wait(0, 1)
    p_spread(1)
    p_relay(0)
    for number, (begin, size) in enumerate(groups):
        for step in (1, 2, 3):
            z_wait(1 + number, step)
        place = pl.ds(pl.multiple_of(me * rows + begin, 16), size)
        for g in range(n_grp):
            amps[place, g * cols:(g + 1) * cols] = pieces[g, begin:begin + size, :]
        p_spread(n_grp + number)
        p_relay(1 if number == 0 else n_grp)
    for step in (3, 2):
        z_wait(0, step)
        p_spread(step)
    p_relay(n_grp + 1)
    p_relay(3)
    for item in (0, 1, n_grp):
        p_across(item)
    p_relay(2)
    for item in (n_grp + 1, 3, 2):
        p_across(item)
    for item in range(first):
        p_rest(item)
    for step in (1, 2, 3):
        z_wait(3, step)

    own = factor[:, rows_of(me, points), :].reshape(n_grp * points, virtuals)
    left[...] = jnp.dot(own, amps[...], preferred_element_type=F32).astype(BF16)
    weighted = []
    for g in range(n_grp):
        products = lax.dot_general(
            left[...], factor[g], (((1,), (1,)), ((), ())), preferred_element_type=F32
        )
        weighted.append((weights[g].astype(F32) * products).astype(BF16))
    weighted = jnp.concatenate(weighted, axis=1)
    total = n_grp * n_blk * points
    for number, (start, width) in enumerate(chunks):
        part = jnp.dot(
            weighted, factor[:, :, start:start + width].reshape(total, width),
            preferred_element_type=F32,
        ).astype(BF16)
        mixed[number, rows_of(me, n_grp * points), :width] = part
        p_spread(first + number)

    picked = lax.broadcasted_iota(jnp.int32, (rows, virtuals), 1) == (
        lax.broadcasted_iota(jnp.int32, (rows, virtuals), 0) + me * rows
    )
    energies = e_ref[...].reshape(1, virtuals)
    first_energy = jnp.sum(jnp.where(picked, energies, 0.0), axis=1, keepdims=True)
    second_energy = jnp.zeros((1, cols), F32)
    for g in range(n_grp):
        second_energy += jnp.where(grp == g, energies[:, g * cols:(g + 1) * cols], 0.0)
    energy_sum = first_energy + second_energy
    picked = picked.astype(F32).astype(BF16)
    by_owner = jnp.concatenate(
        [
            factor[:, block * points:(block + 1) * points, :].reshape(n_grp * points, virtuals)
            for block in range(n_blk)
        ],
        axis=0,
    )
    columns = lax.dot_general(
        picked, by_owner, (((1,), (1,)), ((), ())),
        preferred_element_type=F32,
    ).astype(BF16)

    def o_copy(target, source):
        return pltpu.make_async_remote_copy(
            src_ref=out_send.at[target], dst_ref=out_recv.at[source],
            send_sem=o_send_sem.at[target], recv_sem=o_recv_sem.at[source],
            device_id={"grp": target}, device_id_type=MESH,
        )

    ready = [0]

    def finish(number):
        start, width = chunks[number]
        p_across(first + number)
        p_rest(first + number)
        ladder[:, start:start + width] = jnp.dot(
            columns, mixed[number, :, :width],
            preferred_element_type=F32,
        )
        while ready[0] < n_grp and (ready[0] + 1) * cols <= start + width:
            target = ready[0]
            out_send[target] = ladder[:, target * cols:(target + 1) * cols].astype(BF16)

            @pl.when(grp != target)
            def _(target=target):
                o_copy(target, grp).start()

            ready[0] += 1

    ahead = 3
    for number in range(len(chunks) + ahead - 1):
        if number < len(chunks):
            p_relay(first + number)
        if number >= ahead - 1:
            finish(number - ahead + 1)
    out_recv[grp] = out_send[grp]
    for pair in range(pairs):
        @pl.when(grp != pair)
        def _(pair=pair):
            o_copy(pair, pair).wait_recv()

        diagonal = (energy_sum - f_ref[pair]) * own_amps[pair].astype(F32)
        o_ref[pair] = diagonal + out_recv[pair].astype(F32)
    for target in range(n_grp):
        @pl.when(grp != target)
        def _(target=target):
            o_copy(target, grp).wait_send()
    for copy in started:
        copy.wait_send()


def by_pair(n_blk, n_grp, amplitudes, grid_factor, metric, virt_energy, pair_energy):
    rows, pairs, cols = amplitudes.shape
    points, virtuals = grid_factor.shape
    height, unused, width = metric.shape
    chunks = column_chunks(virtuals, -(-cols // 128) * 128)
    items = n_grp + 2 + len(chunks)
    dma = pltpu.SemaphoreType.DMA
    vmem = pl.BlockSpec(memory_space=pltpu.VMEM)
    residual = pl.pallas_call(
        functools.partial(kernel, n_blk, n_grp),
        out_shape=jax.ShapeDtypeStruct((pairs, rows, cols), F32),
        in_specs=[pl.BlockSpec(memory_space=pltpu.HBM)] * 3 + [vmem, pl.BlockSpec(memory_space=pltpu.SMEM)],
        out_specs=vmem,
        scratch_shapes=[
            pltpu.VMEM(amplitudes.shape, BF16),
            pltpu.VMEM(grid_factor.shape, BF16),
            pltpu.VMEM(metric.shape, F32),
            dma((3,)),
            pltpu.VMEM((pairs, rows, cols), BF16),
            pltpu.VMEM((height, width), BF16),
            pltpu.VMEM((n_grp, n_blk * points, virtuals), BF16),
            pltpu.VMEM((n_grp, rows, cols), BF16),
            pltpu.VMEM((n_blk * rows, virtuals), BF16),
            pltpu.VMEM((n_grp, height, width), BF16),
            pltpu.VMEM((n_grp * points, virtuals), BF16),
            pltpu.VMEM((len(chunks), n_grp * n_blk * points, chunks[0][1]), BF16),
            pltpu.VMEM((rows, virtuals), F32),
            pltpu.VMEM((n_grp, rows, cols), BF16),
            pltpu.VMEM((n_grp, rows, cols), BF16),
            dma((4, n_grp)), dma((4, n_grp)),
            dma((items, 2, n_blk)), dma((items, 2, n_blk)),
            dma((n_grp,)), dma((n_grp,)),
        ],
        compiler_params=pltpu.CompilerParams(collective_id=0, has_side_effects=True),
    )(amplitudes, grid_factor, metric, virt_energy, pair_energy)
    return jnp.transpose(residual, (1, 0, 2))


def solution(mesh):
    in_specs = (P("blk", None, "grp"), P(("blk", "grp"), None), P("blk", "grp", None), P(), P())
    out_specs = P("blk", None, "grp")
    n_blk, n_grp = mesh.shape["blk"], mesh.shape["grp"]

    def body(amplitudes, *rest):
        rows, pairs, cols = amplitudes.shape
        points, virtuals = rest[0].shape
        fits = pairs == n_grp and n_grp == 4 and n_blk == 8
        fits = fits and rows % 16 == 0 and points % 32 == 0 and virtuals % 128 == 0
        if fits:
            return by_pair(n_blk, n_grp, amplitudes, *rest)
        return local(amplitudes, *rest)

    return jax.shard_map(body, mesh=mesh, in_specs=in_specs, out_specs=out_specs, check_vma=False)
```

```python
import functools

import jax
import jax.numpy as jnp
from jax import lax
from jax.experimental import pallas as pl
from jax.experimental.pallas import tpu as pltpu
from jax.sharding import PartitionSpec as P


def local(amplitudes, grid_factor, metric, virt_energy, pair_energy):
    row_factor = lax.all_gather(grid_factor, "grp", axis=0, tiled=True)
    column_factor = lax.all_gather(grid_factor, "blk", axis=0, tiled=True)
    amplitude_rows = lax.all_gather(amplitudes, "blk", axis=0, tiled=True)
    row_count = row_factor.shape[0]
    left_part = jnp.einsum(
        "pc,ckd->kpd", row_factor, amplitude_rows, preferred_element_type=jnp.float32
    ).astype(jnp.bfloat16)
    columns = column_factor
    products = jnp.einsum(
        "kpd,qd->kpq",
        lax.all_gather(left_part, "grp", axis=2, tiled=True),
        columns,
        preferred_element_type=jnp.float32,
    )
    weighted = (metric.reshape(row_count, -1)[None] * products).astype(jnp.bfloat16)
    columns = column_factor
    mixed = lax.psum_scatter(
        jnp.einsum("kpq,qb->bkp", weighted, columns, preferred_element_type=jnp.float32).astype(
            jnp.bfloat16
        ),
        "grp",
        scatter_dimension=0,
        tiled=True,
    )
    columns = row_factor
    ladder = lax.psum_scatter(
        jnp.einsum("pa,bkp->akb", columns, mixed, preferred_element_type=jnp.float32).astype(
            jnp.bfloat16
        ),
        "blk",
        scatter_dimension=0,
        tiled=True,
    ).astype(jnp.float32)
    first_energy = lax.dynamic_slice_in_dim(
        virt_energy, lax.axis_index("blk") * amplitudes.shape[0], amplitudes.shape[0]
    )
    second_energy = lax.dynamic_slice_in_dim(
        virt_energy, lax.axis_index("grp") * amplitudes.shape[2], amplitudes.shape[2]
    )
    denominator = (
        first_energy[:, None, None] + second_energy[None, None, :] - pair_energy[None, :, None]
    )
    return denominator * amplitudes.astype(jnp.float32) + ladder


MESH = pl.DeviceIdType.MESH
F32 = jnp.float32
BF16 = jnp.bfloat16


def flip(index, mask):
    bit = 1
    while bit <= mask:
        if mask & bit:
            index = index + bit - 2 * bit * lax.rem(lax.div(index, bit), 2)
        bit *= 2
    return index


def column_chunks(total, width):
    return [(start, min(width, total - start)) for start in range(0, total, width)]


def kernel(
    n_blk, n_grp, t_hbm, x_hbm, z_hbm, e_ref, f_ref, o_ref,
    t_ref, x_ref, z_ref, in_sem, own_amps, own_weights, factor, pieces, amps, weights, left, mixed, ladder, out_send, out_recv,
    z_send_sem, z_recv_sem, p_send_sem, p_recv_sem, o_send_sem, o_recv_sem,
):
    me = lax.axis_index("blk")
    grp = lax.axis_index("grp")
    rows, pairs, cols = t_ref.shape
    points, virtuals = x_ref.shape
    core, near, far = 1, 2, 4
    direct = [near, far, core]
    started = []

    def peer(step):
        return flip(grp, step)

    barrier = pltpu.get_barrier_semaphore()
    loads = [
        pltpu.make_async_copy(src, dst, in_sem.at[number])
        for number, (src, dst) in enumerate(
            ((t_hbm, t_ref), (z_hbm, z_ref), (x_hbm, x_ref))
        )
    ]
    for load in loads:
        load.start()
    for step in range(1, n_grp):
        pl.semaphore_signal(barrier, inc=1, device_id={"grp": peer(step)}, device_id_type=MESH)
    for mask in direct:
        pl.semaphore_signal(barrier, inc=1, device_id={"blk": flip(me, mask)}, device_id_type=MESH)
    loads[0].wait()
    for pair in range(pairs):
        own_amps[pair] = t_ref[:, pair, :]
    for load in loads[1:]:
        load.wait()
    own_weights[...] = z_ref[:, 0, :].astype(BF16)
    pl.semaphore_wait(barrier, n_grp - 1 + len(direct))

    def rows_of(source, size):
        return pl.ds(pl.multiple_of(source * size, size), size)

    cut = -(-rows // 32) * 16
    groups = ((0, cut), (cut, rows - cut))

    def z_copy(kind, step, src, dst):
        return pltpu.make_async_remote_copy(
            src_ref=src, dst_ref=dst,
            send_sem=z_send_sem.at[kind, step], recv_sem=z_recv_sem.at[kind, step],
            device_id={"grp": peer(step)}, device_id_type=MESH,
        )

    def z_dst(kind, source):
        if kind == 0:
            return factor.at[source, rows_of(me, points), :]
        if kind == 3:
            return weights.at[source]
        begin, size = groups[kind - 1]
        return pieces.at[source, begin:begin + size, :]

    def z_start(kind, step):
        if kind in (1, 2):
            begin, size = groups[kind - 1]
            src = own_amps.at[peer(step), begin:begin + size, :]
        else:
            src = x_ref if kind == 0 else own_weights
        copy = z_copy(kind, step, src, z_dst(kind, grp))
        copy.start()
        started.append(copy)

    def z_wait(kind, step):
        dst = z_dst(kind, peer(step))
        z_copy(kind, step, dst, dst).wait_recv()

    chunks = column_chunks(virtuals, -(-cols // 128) * 128)

    first = n_grp + len(groups)

    def region(item, half, source):
        if item < n_grp:
            part = points // 2
            begin = pl.multiple_of(source * points + half * part, part)
            return factor.at[peer(item), pl.ds(begin, part), :]
        if item < first:
            begin, size = groups[item - n_grp]
            part = -(-size // 32) * 16
            begin += half * part + source * rows
            return amps.at[pl.ds(pl.multiple_of(begin, 16), part if half == 0 else size - part), :]
        number = item - first
        part = n_grp * points // 2
        begin = pl.multiple_of(source * 2 * part + half * part, part)
        return mixed.at[number, pl.ds(begin, part), pl.ds(0, chunks[number][1])]

    def p_copy(item, half, mask, hop, src=None):
        place = region(item, half, flip(me, mask))
        return pltpu.make_async_remote_copy(
            src_ref=place if src is None else src, dst_ref=place,
            send_sem=p_send_sem.at[item, half, mask ^ hop],
            recv_sem=p_recv_sem.at[item, half, mask ^ hop],
            device_id={"blk": flip(me, hop)}, device_id_type=MESH,
        )

    def p_send(item, half, mask, hop, src=None):
        copy = p_copy(item, half, mask, hop, src)
        copy.start()
        started.append(copy)

    def p_wait(item, half, mask):
        p_copy(item, half, mask, 0).wait_recv()

    def relayed(item):
        return item not in (2, first + len(chunks) - 1)

    def p_spread(item, src=None):
        sources = (None, None)
        if src is not None:
            part = points // 2
            sources = tuple(src.at[half * part:(half + 1) * part, :] for half in range(2))
        for turn in range(2):
            p_send(item, turn, 0, near, sources[turn])
            p_send(item, 1 - turn, 0, far, sources[1 - turn])
        if not relayed(item):
            for half in range(2):
                p_send(item, half, 0, near + far, sources[half])
        for half in range(2):
            p_send(item, half, 0, core, sources[half])

    def p_relay(item):
        for turn in range(2):
            for mask, half, onward in ((near, turn, far), (far, 1 - turn, near)):
                p_wait(item, half, mask)
                if turn == 0 and relayed(item):
                    p_send(item, half, mask, onward)
                p_send(item, half, mask, core)

    def p_across(item):
        for half in range(2):
            p_wait(item, half, near + far)
            p_send(item, half, near + far, core)

    def p_rest(item):
        for mask in range(1, n_blk, 2):
            for half in range(2):
                p_wait(item, half, mask)

    p_spread(0, x_ref)
    z_start(0, 1)
    for kind in (1, 2):
        for step in (1, 2, 3):
            z_start(kind, step)
    z_start(0, 3)
    z_start(0, 2)
    for step in (1, 2, 3):
        z_start(3, step)
    factor[grp, rows_of(me, points), :] = x_ref[...]
    pieces[grp] = own_amps[grp]
    weights[grp] = own_weights[...]
    z_wait(0, 1)
    p_spread(1)
    p_relay(0)
    for number, (begin, size) in enumerate(groups):
        for step in (1, 2, 3):
            z_wait(1 + number, step)
        place = pl.ds(pl.multiple_of(me * rows + begin, 16), size)
        for g in range(n_grp):
            amps[place, g * cols:(g + 1) * cols] = pieces[g, begin:begin + size, :]
        p_spread(n_grp + number)
        p_relay(1 if number == 0 else n_grp)
    for step in (3, 2):
        z_wait(0, step)
        p_spread(step)
    p_relay(n_grp + 1)
    p_relay(3)
    for item in (0, 1, n_grp):
        p_across(item)
    p_relay(2)
    for item in (n_grp + 1, 3, 2):
        p_across(item)
    for item in range(first):
        p_rest(item)
    for step in (1, 2, 3):
        z_wait(3, step)

    own = factor[:, rows_of(me, points), :].reshape(n_grp * points, virtuals)
    left[...] = jnp.dot(own, amps[...], preferred_element_type=F32).astype(BF16)
    weighted = []
    for g in range(n_grp):
        products = lax.dot_general(
            left[...], factor[g], (((1,), (1,)), ((), ())), preferred_element_type=F32
        )
        weighted.append((weights[g].astype(F32) * products).astype(BF16))
    weighted = jnp.concatenate(weighted, axis=1)
    total = n_grp * n_blk * points
    for number, (start, width) in enumerate(chunks):
        part = jnp.dot(
            weighted, factor[:, :, start:start + width].reshape(total, width),
            preferred_element_type=F32,
        ).astype(BF16)
        mixed[number, rows_of(me, n_grp * points), :width] = part
        p_spread(first + number)

    picked = lax.broadcasted_iota(jnp.int32, (rows, virtuals), 1) == (
        lax.broadcasted_iota(jnp.int32, (rows, virtuals), 0) + me * rows
    )
    energies = e_ref[...].reshape(1, virtuals)
    first_energy = jnp.sum(jnp.where(picked, energies, 0.0), axis=1, keepdims=True)
    second_energy = jnp.zeros((1, cols), F32)
    for g in range(n_grp):
        second_energy += jnp.where(grp == g, energies[:, g * cols:(g + 1) * cols], 0.0)
    energy_sum = first_energy + second_energy
    picked = picked.astype(F32).astype(BF16)
    by_owner = jnp.concatenate(
        [
            factor[:, block * points:(block + 1) * points, :].reshape(n_grp * points, virtuals)
            for block in range(n_blk)
        ],
        axis=0,
    )
    columns = lax.dot_general(
        picked, by_owner, (((1,), (1,)), ((), ())),
        preferred_element_type=F32,
    ).astype(BF16)

    def o_copy(target, source):
        return pltpu.make_async_remote_copy(
            src_ref=out_send.at[target], dst_ref=out_recv.at[source],
            send_sem=o_send_sem.at[target], recv_sem=o_recv_sem.at[source],
            device_id={"grp": target}, device_id_type=MESH,
        )

    ready = [0]

    def finish(number):
        start, width = chunks[number]
        p_across(first + number)
        p_rest(first + number)
        ladder[:, start:start + width] = jnp.dot(
            columns, mixed[number, :, :width],
            preferred_element_type=F32,
        )
        while ready[0] < n_grp and (ready[0] + 1) * cols <= start + width:
            target = ready[0]
            out_send[target] = ladder[:, target * cols:(target + 1) * cols].astype(BF16)

            @pl.when(grp != target)
            def _(target=target):
                o_copy(target, grp).start()

            ready[0] += 1

    ahead = 4
    for number in range(len(chunks) + ahead - 1):
        if number < len(chunks):
            p_relay(first + number)
        if number >= ahead - 1:
            finish(number - ahead + 1)
    out_recv[grp] = out_send[grp]
    for pair in range(pairs):
        @pl.when(grp != pair)
        def _(pair=pair):
            o_copy(pair, pair).wait_recv()

        diagonal = (energy_sum - f_ref[pair]) * own_amps[pair].astype(F32)
        o_ref[pair] = diagonal + out_recv[pair].astype(F32)
    for target in range(n_grp):
        @pl.when(grp != target)
        def _(target=target):
            o_copy(target, grp).wait_send()
    for copy in started:
        copy.wait_send()


def by_pair(n_blk, n_grp, amplitudes, grid_factor, metric, virt_energy, pair_energy):
    rows, pairs, cols = amplitudes.shape
    points, virtuals = grid_factor.shape
    height, unused, width = metric.shape
    chunks = column_chunks(virtuals, -(-cols // 128) * 128)
    items = n_grp + 2 + len(chunks)
    dma = pltpu.SemaphoreType.DMA
    vmem = pl.BlockSpec(memory_space=pltpu.VMEM)
    residual = pl.pallas_call(
        functools.partial(kernel, n_blk, n_grp),
        out_shape=jax.ShapeDtypeStruct((pairs, rows, cols), F32),
        in_specs=[pl.BlockSpec(memory_space=pltpu.HBM)] * 3 + [vmem, pl.BlockSpec(memory_space=pltpu.SMEM)],
        out_specs=vmem,
        scratch_shapes=[
            pltpu.VMEM(amplitudes.shape, BF16),
            pltpu.VMEM(grid_factor.shape, BF16),
            pltpu.VMEM(metric.shape, F32),
            dma((3,)),
            pltpu.VMEM((pairs, rows, cols), BF16),
            pltpu.VMEM((height, width), BF16),
            pltpu.VMEM((n_grp, n_blk * points, virtuals), BF16),
            pltpu.VMEM((n_grp, rows, cols), BF16),
            pltpu.VMEM((n_blk * rows, virtuals), BF16),
            pltpu.VMEM((n_grp, height, width), BF16),
            pltpu.VMEM((n_grp * points, virtuals), BF16),
            pltpu.VMEM((len(chunks), n_grp * n_blk * points, chunks[0][1]), BF16),
            pltpu.VMEM((rows, virtuals), F32),
            pltpu.VMEM((n_grp, rows, cols), BF16),
            pltpu.VMEM((n_grp, rows, cols), BF16),
            dma((4, n_grp)), dma((4, n_grp)),
            dma((items, 2, n_blk)), dma((items, 2, n_blk)),
            dma((n_grp,)), dma((n_grp,)),
        ],
        compiler_params=pltpu.CompilerParams(collective_id=0, has_side_effects=True),
    )(amplitudes, grid_factor, metric, virt_energy, pair_energy)
    return jnp.transpose(residual, (1, 0, 2))


def solution(mesh):
    in_specs = (P("blk", None, "grp"), P(("blk", "grp"), None), P("blk", "grp", None), P(), P())
    out_specs = P("blk", None, "grp")
    n_blk, n_grp = mesh.shape["blk"], mesh.shape["grp"]

    def body(amplitudes, *rest):
        rows, pairs, cols = amplitudes.shape
        points, virtuals = rest[0].shape
        fits = pairs == n_grp and n_grp == 4 and n_blk == 8
        fits = fits and rows % 16 == 0 and points % 32 == 0 and virtuals % 128 == 0
        if fits:
            return by_pair(n_blk, n_grp, amplitudes, *rest)
        return local(amplitudes, *rest)

    return jax.shard_map(body, mesh=mesh, in_specs=in_specs, out_specs=out_specs, check_vma=False)
```
